8 devices in a mesh: dp: 2 (over z, y), tp: 4 (over x, core).
Axes of the slice: x: 2, y: 2, z: 1, core: 2. Of those that a mesh axis runs over, the one named last changes fastest.
Arguments:
- enc_out: bfloat16 [12, 2048, 2048], P('dp', 'tp'), parts along dimension 0
- norm_scale: bfloat16 [2048], replicated
- w_key: bfloat16 [6, 2048, 32, 64], P(None, None, 'tp')
- w_value: bfloat16 [6, 2048, 32, 64], P(None, None, 'tp')
Outputs:
- output 1: bfloat16 [6, 12, 2048, 32, 64], P(None, 'dp', None, 'tp'), parts along dimension 1
- output 2: bfloat16 [6, 12, 2048, 32, 64], P(None, 'dp', None, 'tp'), parts along dimension 1
There are 2 independent parts. The reference program is written for one: setup_inputs(seed, part) draws one part's arguments, and reference() takes and returns one part's arrays. A program takes and returns all parts, laid end to end along the dimension named above; an argument that names none is the same for every part.
All inputs are finite; a program needn't handle non-finite values.
Results may differ from the reference program's by a relative error of at most 0.001.
Values are sent between devices in bfloat16 or wider.
A program may use at most 1 GiB of HBM per device.

```python
import jax
import jax.numpy as jnp
from jax import lax

N_LAYERS = 6
BATCH_SIZE = 6
SEQ_LEN = 2048
D_MODEL = 2048
N_HEADS = 32
HEAD_DIM = 64
NORM_EPS = 1e-6


def setup_inputs(seed: int = 0, part: int = 0) -> dict:
    root_key = jax.random.key(seed)
    k_act, k_norm, k_key, k_val = jax.random.split(root_key, 4)
    k_act = jax.random.fold_in(k_act, part)
    w_scale = D_MODEL ** -0.5
    w_shape = (N_LAYERS, D_MODEL, N_HEADS, HEAD_DIM)
    enc_out = jax.random.normal(k_act, (BATCH_SIZE, SEQ_LEN, D_MODEL), jnp.float32)
    norm_scale = jax.random.uniform(k_norm, (D_MODEL,), jnp.float32, 0.5, 1.5)
    w_key = jax.random.normal(k_key, w_shape, jnp.float32) * w_scale
    w_value = jax.random.normal(k_val, w_shape, jnp.float32) * w_scale
    return {"enc_out": enc_out.astype(jnp.bfloat16), "norm_scale": norm_scale.astype(jnp.bfloat16), "w_key": w_key.astype(jnp.bfloat16), "w_value": w_value.astype(jnp.bfloat16)}


def rms_norm(enc_out, norm_scale):
    acts = enc_out.astype(jnp.float32)
    mean_sq = jnp.mean(acts * acts, axis=-1, keepdims=True)
    return (acts * lax.rsqrt(mean_sq + NORM_EPS) * norm_scale.astype(jnp.float32)).astype(jnp.bfloat16)


def reference(enc_out, norm_scale, w_key, w_value):
    normed = rms_norm(enc_out, norm_scale).reshape(BATCH_SIZE * SEQ_LEN, D_MODEL)
    out_shape = (BATCH_SIZE, SEQ_LEN, N_HEADS, HEAD_DIM)

    def project(layer_weights):
        layer_key, layer_value = layer_weights
        keys = jnp.dot(normed, layer_key.reshape(D_MODEL, N_HEADS * HEAD_DIM), preferred_element_type=jnp.float32)
        values = jnp.dot(normed, layer_value.reshape(D_MODEL, N_HEADS * HEAD_DIM), preferred_element_type=jnp.float32)
        return keys.astype(jnp.bfloat16).reshape(out_shape), values.astype(jnp.bfloat16).reshape(out_shape)

    key_cache, value_cache = lax.map(project, (w_key, w_value))
    return key_cache, value_cache
```

```python
import functools
import jax, jax.numpy as jnp
from jax import lax
from jax.experimental import pallas as pl
from jax.experimental.pallas import tpu as pltpu

from jax.sharding import PartitionSpec as P

NORM_EPS = 1e-6
L, D, HK, TOK = 6, 2048, 512, 512
PIECES, ROWS = 4, 128
NT = D // 256

def proj_body(units, n_src, has_prev, *refs):
    n = len(units)
    srcs = refs[:n_src]
    wk, wv = refs[n_src:n_src + 2]
    ok, ov = refs[n_src + 2 + (2 if has_prev else 0):n_src + 4 + (2 if has_prev else 0)]
    ybuf, wbuf, obuf, y_sem, w_sem, o_sem = refs[-6:]
    me = lax.axis_index("tp")

    def out_copy(kv, t, slot):
        t = jnp.maximum(t, 0)
        layer, u = t // n, t % n
        seq, code = unit_scalars(u)
        other = jnp.bitwise_xor(me, code)
        dst = (ok, ov)[kv].at[layer, seq, :, pl.ds(pl.multiple_of(other * TOK, TOK), TOK)]
        return pltpu.make_async_copy(obuf.at[kv, slot], dst, o_sem.at[kv])

    def unit_scalars(u):
        seq, code = jnp.int32(units[0][2]), jnp.int32(units[0][3])
        for i in range(1, n):
            seq = jnp.where(u == i, units[i][2], seq)
            code = jnp.where(u == i, units[i][3], code)
        return seq, code

    def w_copy(kv, layer, slot):
        return pltpu.make_async_copy((wk, wv)[kv].at[layer], wbuf.at[slot, kv], w_sem.at[slot, kv])

    def y_copy(u):
        s, i = units[u][:2]
        return pltpu.make_async_copy(srcs[s].at[i], ybuf.at[u], y_sem.at[u])

    def y_wait(u):
        pltpu.make_async_copy(srcs[0].at[0], ybuf.at[u], y_sem.at[u]).wait()

    def run(*accs):
        acc = [[[accs[(kv * 2 + q) * PIECES + p] for p in range(PIECES)] for q in range(2)] for kv in range(2)]

        def push(u, tile, reg):
            for q in range(2):
                pltpu.matmul_push_rhs(ybuf[u, pl.ds(q * 256, 256), pl.ds(tile * 256, 256)], staging_register=reg, mxu_index=q, transpose=True)

        def feed(kv, slot, tile, reg):
            for p in range(PIECES):
                lhs = wbuf[slot, kv, pl.ds(p * ROWS, ROWS), pl.ds(tile * 256, 256)]
                for q in range(2):
                    pltpu.matmul_acc_lhs(acc[kv][q][p], lhs, load_staged_rhs=reg if p == 0 else None)

        def drain(kv, p, slot):
            for q in range(2):
                obuf[kv, slot, pl.ds(p * ROWS, ROWS), pl.ds(q * 256, 256)] = pltpu.matmul_pop(acc[kv][q][p]).astype(jnp.bfloat16)

        w_copy(0, 0, 0).start()
        y_copy(0).start()
        w_copy(1, 0, 0).start()
        for u in range(1, n):
            y_copy(u).start()
        out_copy(0, 0, 0).start()
        out_copy(1, 0, 0).start()
        y_copy(0).wait()
        for kv in range(2):
            for p in range(PIECES):
                drain(kv, p, 1)
        push(0, 0, 1)
        for p in range(PIECES):
            for q in range(2):
                pltpu.matmul_acc_lhs(acc[1][q][p], jnp.zeros((ROWS, 256), jnp.bfloat16), load_staged_rhs=1 if p == 0 else None)
        push(0, 0, 0)

        def trip(layer, u, first):
            t = layer * n + u
            slot, oslot = layer % 2, t % 2
            out_copy(0, t - 2, 0).wait()
            out_copy(1, t - 3, 0).wait()
            out_copy(0, t - 1, 1 - oslot).start()
            out_copy(1, t - 2, oslot).start()
            if first:
                @pl.when(u + 1 < n)
                def _():
                    y_wait(u + 1)
            nxt = lax.rem(u + 1, n)
            for i in range(2 * NT):
                kv, tile = divmod(i, NT)
                feed(kv, slot, tile, i % 2)
                if i < 2 * NT - 1:
                    push(u, (i + 1) % NT, (i + 1) % 2)
                else:
                    push(nxt, 0, 0)
                if 1 <= tile <= PIECES:
                    drain(1 - kv, tile - 1, 1 - oslot if kv == 0 else oslot)

        for layer in range(1):
            for kv in range(2):
                w_copy(kv, 0, 0).wait()
            for kv in range(2):
                w_copy(kv, 1, 1).start()
        lax.fori_loop(0, n, lambda u, c: (trip(0, u, True), c)[1], 0)

        def layer_loop(layer, c):
            slot = layer % 2
            for kv in range(2):
                w_copy(kv, layer, slot).wait()
            nl = jnp.minimum(layer + 1, L - 1)
            for kv in range(2):
                w_copy(kv, nl, 1 - slot).start()
            lax.fori_loop(0, n, lambda u, c: (trip(layer, u, False), c)[1], 0)
            return c
        lax.fori_loop(1, L, layer_loop, 0)
        T = L * n
        for kv in range(2):
            w_copy(kv, L - 1, L % 2).wait()
        out_copy(0, T - 2, 0).wait()
        out_copy(1, T - 3, 0).wait()
        out_copy(0, T - 1, (T - 1) % 2).start()
        out_copy(1, T - 2, (T - 2) % 2).start()
        for p in range(PIECES):
            drain(1, p, (T - 1) % 2)
        out_copy(1, T - 2, 0).wait()
        out_copy(1, T - 1, (T - 1) % 2).start()
        out_copy(0, T - 1, 0).wait()
        out_copy(1, T - 1, 0).wait()
        for p in range(PIECES):
            for q in range(2):
                pltpu.matmul_acc_lhs(acc[0][q][p], jnp.zeros((ROWS, 256), jnp.bfloat16), load_staged_rhs=0 if p == 0 else None)

    pl.run_scoped(run, *[pltpu.ACC(q)((ROWS, 256), jnp.float32) for kv in range(2) for q in range(2) for p in range(PIECES)])

def project(sources, units, wk, wv, prev):
    n = len(units)
    out = jax.ShapeDtypeStruct((L, 6, HK, 4 * TOK), jnp.bfloat16)
    args = list(sources) + [wk, wv] + (list(prev) if prev else [])
    k = len(sources) + 2
    return pl.pallas_call(
        functools.partial(proj_body, units, len(sources), bool(prev)),
        out_shape=[out, out],
        in_specs=[pl.BlockSpec(memory_space=pl.ANY)] * len(args),
        out_specs=[pl.BlockSpec(memory_space=pl.ANY)] * 2,
        scratch_shapes=[
            pltpu.VMEM((n, TOK, D), jnp.bfloat16),
            pltpu.VMEM((2, 2, HK, D), jnp.bfloat16),
            pltpu.VMEM((2, 2, HK, TOK), jnp.bfloat16),
            pltpu.SemaphoreType.DMA((n,)),
            pltpu.SemaphoreType.DMA((2, 2)),
            pltpu.SemaphoreType.DMA((2,)),
        ],
        input_output_aliases={k: 0, k + 1: 1} if prev else {},
        cost_estimate=pl.CostEstimate(flops=2 * n * TOK * D * HK * 2 * L, bytes_accessed=n * (TOK * D * 2 + 2 * L * HK * TOK * 2) + 4 * L * HK * D, transcendentals=0),
        compiler_params=pltpu.CompilerParams(vmem_limit_bytes=48 * 1024 * 1024, has_side_effects=True),
    )(*args)


def PLAN(me, mt, fr, fw):
    return [me, mt + fr[:1], fw[:1] + fr[1:4], fw[1:4] + fr[4:5], fw[4:5] + fr[5:], fw[5:]]


def rms_norm(enc_out, norm_scale):
    acts = enc_out.astype(jnp.float32)
    mean_sq = jnp.mean(acts * acts, axis=-1, keepdims=True)
    return (acts * lax.rsqrt(mean_sq + NORM_EPS) * norm_scale.astype(jnp.float32)).astype(jnp.bfloat16)


def swap(x, code):
    return lax.ppermute(x, "tp", [(i, i ^ code) for i in range(4)])


def solution(mesh):
    def per_device(enc_out, norm_scale, w_key, w_value):
        wk = jnp.transpose(w_key, (0, 2, 3, 1)).reshape(L, HK, D)
        wv = jnp.transpose(w_value, (0, 2, 3, 1)).reshape(L, HK, D)
        y = [rms_norm(enc_out[c : c + 1], norm_scale) for c in range(6)]
        far = [swap(y[c], 2) for c in range(6)]
        mate = [swap(y[c], 1) for c in range(6)]
        fwd = [swap(far[c], 1) for c in range(6)]
        me, mt, fr, fw = [[[src[c], (c, code)] for c in range(6)] for src, code in ((y, 0), (mate, 1), (far, 2), (fwd, 3))]
        plan = PLAN(me, mt, fr, fw)
        out = None
        for group in plan:
            sources = [g[0] for g in group]
            units = [(i, 0, *g[1]) for i, g in enumerate(group)]
            out = project(sources, units, wk, wv, out)
        return tuple(jnp.transpose(o.reshape(L, 6, 8, 64, 4 * TOK), (0, 1, 4, 2, 3)) for o in out)

    weight_spec = P(None, None, "tp", None)
    cache_spec = P(None, "dp", None, "tp", None)
    return jax.shard_map(per_device, mesh=mesh, in_specs=(P("dp", "tp", None), P(None), weight_spec, weight_spec), out_specs=(cache_spec, cache_spec), check_vma=False)
```

```python
import functools
import jax, jax.numpy as jnp
from jax import lax
from jax.experimental import pallas as pl
from jax.experimental.pallas import tpu as pltpu

from jax.sharding import PartitionSpec as P

NORM_EPS = 1e-6
L, D, HK, TOK = 6, 2048, 512, 512
PIECES, ROWS = 4, 128
NT = D // 256


def proj_body(units, n_src, has_prev, *refs):
    n = len(units)
    srcs = refs[:n_src]
    wk, wv = refs[n_src:n_src + 2]
    ok, ov = refs[n_src + 2 + (2 if has_prev else 0):n_src + 4 + (2 if has_prev else 0)]
    ybuf, wbuf, obuf, y_sem, w_sem, o_sem = refs[-6:]
    me = lax.axis_index("tp")

    def out_copy(kv, t, slot):
        t = jnp.maximum(t, 0)
        layer, u = t // n, t % n
        seq, code = unit_scalars(u)
        other = jnp.bitwise_xor(me, code)
        dst = (ok, ov)[kv].at[layer, seq, :, pl.ds(pl.multiple_of(other * TOK, TOK), TOK)]
        return pltpu.make_async_copy(obuf.at[kv, slot], dst, o_sem.at[kv])

    def unit_scalars(u):
        seq, code = jnp.int32(units[0][2]), jnp.int32(units[0][3])
        for i in range(1, n):
            seq = jnp.where(u == i, units[i][2], seq)
            code = jnp.where(u == i, units[i][3], code)
        return seq, code

    def w_copy(kv, layer, slot):
        return pltpu.make_async_copy((wk, wv)[kv].at[layer], wbuf.at[slot, kv], w_sem.at[slot, kv])

    def y_copy(u):
        s, i = units[u][:2]
        return pltpu.make_async_copy(srcs[s].at[i], ybuf.at[u], y_sem.at[u])

    def y_wait(u):
        pltpu.make_async_copy(srcs[0].at[0], ybuf.at[u], y_sem.at[u]).wait()

    def run(*accs):
        acc = [[[accs[(kv * 2 + q) * PIECES + p] for p in range(PIECES)] for q in range(2)] for kv in range(2)]

        def push(u, tile, reg):
            for q in range(2):
                pltpu.matmul_push_rhs(ybuf[u, pl.ds(q * 256, 256), pl.ds(tile * 256, 256)], staging_register=reg, mxu_index=q, transpose=True)

        def feed(kv, slot, tile, reg):
            for p in range(PIECES):
                lhs = wbuf[slot, kv, pl.ds(p * ROWS, ROWS), pl.ds(tile * 256, 256)]
                for q in range(2):
                    pltpu.matmul_acc_lhs(acc[kv][q][p], lhs, load_staged_rhs=reg if p == 0 else None)

        def drain(kv, p, slot):
            for q in range(2):
                obuf[kv, slot, pl.ds(p * ROWS, ROWS), pl.ds(q * 256, 256)] = pltpu.matmul_pop(acc[kv][q][p]).astype(jnp.bfloat16)

        w_copy(0, 0, 0).start()
        y_copy(0).start()
        w_copy(1, 0, 0).start()
        for u in range(1, n):
            y_copy(u).start()
        out_copy(0, 0, 0).start()
        out_copy(1, 0, 0).start()
        y_copy(0).wait()
        for kv in range(2):
            for p in range(PIECES):
                drain(kv, p, 1)
        push(0, 0, 1)
        for p in range(PIECES):
            for q in range(2):
                pltpu.matmul_acc_lhs(acc[1][q][p], jnp.zeros((ROWS, 256), jnp.bfloat16), load_staged_rhs=1 if p == 0 else None)
        push(0, 0, 0)

        def trip(layer, u, first):
            t = layer * n + u
            slot, oslot = layer % 2, t % 2
            out_copy(0, t - 2, 0).wait()
            out_copy(1, t - 3, 0).wait()
            out_copy(0, t - 1, 1 - oslot).start()
            out_copy(1, t - 2, oslot).start()
            if first:
                @pl.when(u + 1 < n)
                def _():
                    y_wait(u + 1)
            nxt = lax.rem(u + 1, n)
            for i in range(2 * NT):
                kv, tile = divmod(i, NT)
                feed(kv, slot, tile, i % 2)
                if i < 2 * NT - 1:
                    push(u, (i + 1) % NT, (i + 1) % 2)
                else:
                    push(nxt, 0, 0)
                if 1 <= tile <= PIECES:
                    drain(1 - kv, tile - 1, 1 - oslot if kv == 0 else oslot)

        for _ in range(1):
            for kv in range(2):
                w_copy(kv, 0, 0).wait()
            for kv in range(2):
                w_copy(kv, 1, 1).start()
        lax.fori_loop(0, n, lambda u, c: (trip(0, u, True), c)[1], 0)

        def layer_loop(layer, c):
            slot = layer % 2
            for kv in range(2):
                w_copy(kv, layer, slot).wait()
            nl = jnp.minimum(layer + 1, L - 1)
            for kv in range(2):
                w_copy(kv, nl, 1 - slot).start()
            lax.fori_loop(0, n, lambda u, c: (trip(layer, u, False), c)[1], 0)
            return c

        lax.fori_loop(1, L, layer_loop, 0)
        T = L * n
        for kv in range(2):
            w_copy(kv, L - 1, L % 2).wait()
        out_copy(0, T - 2, 0).wait()
        out_copy(1, T - 3, 0).wait()
        out_copy(0, T - 1, (T - 1) % 2).start()
        out_copy(1, T - 2, (T - 2) % 2).start()
        for p in range(PIECES):
            drain(1, p, (T - 1) % 2)
        out_copy(1, T - 2, 0).wait()
        out_copy(1, T - 1, (T - 1) % 2).start()
        out_copy(0, T - 1, 0).wait()
        out_copy(1, T - 1, 0).wait()
        for p in range(PIECES):
            for q in range(2):
                pltpu.matmul_acc_lhs(acc[0][q][p], jnp.zeros((ROWS, 256), jnp.bfloat16), load_staged_rhs=0 if p == 0 else None)

    pl.run_scoped(run, *[pltpu.ACC(q)((ROWS, 256), jnp.float32) for _ in range(2) for q in range(2) for _ in range(PIECES)])


def project(sources, units, wk, wv, prev):
    n = len(units)
    out = jax.ShapeDtypeStruct((L, 6, HK, 4 * TOK), jnp.bfloat16)
    args = list(sources) + [wk, wv] + (list(prev) if prev else [])
    k = len(sources) + 2
    return pl.pallas_call(
        functools.partial(proj_body, units, len(sources), bool(prev)),
        out_shape=[out, out],
        in_specs=[pl.BlockSpec(memory_space=pl.ANY)] * len(args),
        out_specs=[pl.BlockSpec(memory_space=pl.ANY)] * 2,
        scratch_shapes=[
            pltpu.VMEM((n, TOK, D), jnp.bfloat16),
            pltpu.VMEM((2, 2, HK, D), jnp.bfloat16),
            pltpu.VMEM((2, 2, HK, TOK), jnp.bfloat16),
            pltpu.SemaphoreType.DMA((n,)),
            pltpu.SemaphoreType.DMA((2, 2)),
            pltpu.SemaphoreType.DMA((2,)),
        ],
        input_output_aliases={k: 0, k + 1: 1} if prev else {},
        cost_estimate=pl.CostEstimate(flops=2 * n * TOK * D * HK * 2 * L, bytes_accessed=n * (TOK * D * 2 + 2 * L * HK * TOK * 2) + 4 * L * HK * D, transcendentals=0),
        compiler_params=pltpu.CompilerParams(vmem_limit_bytes=60 * 1024 * 1024, has_side_effects=True),
    )(*args)


def units_of(name, *chunks):
    return [(name, c) for c in chunks]


PLAN = [
    (units_of("own", *range(6)), (0,)),
    (units_of("mate", *range(6)) + units_of("far", 0), (1, 2, 3)),
    (units_of("fwd", 0) + units_of("far", 1, 2, 3), (4,)),
    (units_of("fwd", 1, 2, 3) + units_of("far", 4), (5,)),
    (units_of("fwd", 4) + units_of("far", 5), ()),
    (units_of("fwd", 5), ()),
]


def rms_norm(enc_out, norm_scale):
    acts = enc_out.astype(jnp.float32)
    mean_sq = jnp.mean(acts * acts, axis=-1, keepdims=True)
    return (acts * lax.rsqrt(mean_sq + NORM_EPS) * norm_scale.astype(jnp.float32)).astype(jnp.bfloat16)


def swap(x, code):
    return lax.ppermute(x, "tp", [(i, i ^ code) for i in range(4)])


def solution(mesh):
    def gather_and_project(enc_out, norm_scale, w_key, w_value):
        wk = jnp.transpose(w_key, (0, 2, 3, 1)).reshape(L, HK, D)
        wv = jnp.transpose(w_value, (0, 2, 3, 1)).reshape(L, HK, D)
        y = [rms_norm(enc_out[c : c + 1], norm_scale) for c in range(6)]
        far = [swap(y[c], 2) for c in range(6)]
        mate = [swap(y[c], 1) for c in range(6)]
        fwd = [None] * 6
        kept = {"own": y, "mate": mate, "far": far, "fwd": fwd}
        code = {"own": 0, "mate": 1, "far": 2, "fwd": 3}
        out = None
        for group, forward in PLAN:
            sources = [kept[name][c] for name, c in group]
            units = [(i, 0, c, code[name]) for i, (name, c) in enumerate(group)]
            out = project(sources, units, wk, wv, out)
            if forward:
                out, moved = lax.optimization_barrier((out, [far[c] for c in forward]))
                for c, block in zip(forward, moved):
                    far[c] = block
                    fwd[c] = swap(block, 1)
        return tuple(jnp.transpose(o.reshape(L, 6, 8, 64, 4 * TOK), (0, 1, 4, 2, 3)) for o in out)

    weight_spec = P(None, None, "tp", None)
    cache_spec = P(None, "dp", None, "tp", None)
    return jax.shard_map(gather_and_project, mesh=mesh, in_specs=(P("dp", "tp", None), P(None), weight_spec, weight_spec), out_specs=(cache_spec, cache_spec), check_vma=False)
```

```python
import functools
import jax, jax.numpy as jnp
from jax import lax
from jax.experimental import pallas as pl
from jax.experimental.pallas import tpu as pltpu

from jax.sharding import PartitionSpec as P

NORM_EPS = 1e-6
L, D, HK, TOK = 6, 2048, 512, 512
PIECES, ROWS = 8, 64
SPREAD = 2
NT = D // 256


def proj_body(units, n_src, has_prev, *refs):
    n = len(units)
    srcs = refs[:n_src]
    wk, wv = refs[n_src:n_src + 2]
    ok, ov = refs[n_src + 2 + (2 if has_prev else 0):n_src + 4 + (2 if has_prev else 0)]
    ybuf, wbuf, obuf, y_sem, w_sem, o_sem = refs[-6:]
    me = lax.axis_index("tp")

    def place(layer, u):
        seq, code = unit_scalars(u)
        return layer, seq, jnp.bitwise_xor(me, code) * TOK

    def out_copy(kv, at, slot):
        layer, seq, col = at
        dst = (ok, ov)[kv].at[layer, seq, :, pl.ds(pl.multiple_of(col, TOK), TOK)]
        return pltpu.make_async_copy(obuf.at[kv, slot], dst, o_sem.at[kv])

    def unit_scalars(u):
        seq, code = jnp.int32(units[0][2]), jnp.int32(units[0][3])
        for i in range(1, n):
            seq = jnp.where(u == i, units[i][2], seq)
            code = jnp.where(u == i, units[i][3], code)
        return seq, code

    def w_copy(kv, layer, slot):
        return pltpu.make_async_copy((wk, wv)[kv].at[layer], wbuf.at[slot, kv], w_sem.at[slot, kv])

    def y_copy(u):
        s, i = units[u][:2]
        return pltpu.make_async_copy(srcs[s].at[i], ybuf.at[u], y_sem.at[u])

    def y_wait(u):
        pltpu.make_async_copy(srcs[0].at[0], ybuf.at[u], y_sem.at[u]).wait()

    def run(*accs):
        acc = [[[accs[(kv * 2 + q) * PIECES + p] for p in range(PIECES)] for q in range(2)] for kv in range(2)]

        def push(u, tile, reg):
            for q in range(2):
                pltpu.matmul_push_rhs(ybuf[u, pl.ds(q * 256, 256), pl.ds(tile * 256, 256)], staging_register=reg, mxu_index=q, transpose=True)

        def feed(kv, slot, tile, reg, after):
            for p in range(PIECES):
                lhs = wbuf[slot, kv, pl.ds(p * ROWS, ROWS), pl.ds(tile * 256, 256)]
                for q in range(2):
                    pltpu.matmul_acc_lhs(acc[kv][q][p], lhs, load_staged_rhs=reg if p == 0 else None)
                after(p)

        def drain(kv, p, slot):
            for q in range(2):
                obuf[kv, slot, pl.ds(p * ROWS, ROWS), pl.ds(q * 256, 256)] = pltpu.matmul_pop(acc[kv][q][p]).astype(jnp.bfloat16)

        first = place(0, 0)
        w_copy(0, 0, 0).start()
        y_copy(0).start()
        w_copy(1, 0, 0).start()
        for kv in range(2):
            for p in range(PIECES):
                drain(kv, p, 1)
        out_copy(0, first, 0).start()
        out_copy(1, first, 0).start()
        w_copy(0, 0, 0).wait()
        y_copy(0).wait()
        push(0, 0, 1)
        for p in range(PIECES):
            for q in range(2):
                pltpu.matmul_acc_lhs(acc[1][q][p], jnp.zeros((ROWS, 256), jnp.bfloat16), load_staged_rhs=1 if p == 0 else None)
        push(0, 0, 0)
        for u in range(1, min(n, 2)):
            y_copy(u).start()

        def trip(layer, u, carry, opening):
            last, before = carry
            slot, oslot = layer % 2, (layer * n + u) % 2
            out_copy(0, last, 0).wait()
            out_copy(1, last, 0).wait()
            out_copy(0, last, 1 - oslot).start()
            out_copy(1, before, oslot).start()
            nxt = lax.select(u + 1 == n, 0, u + 1)
            for i in range(2 * NT):
                kv, tile = divmod(i, NT)
                if opening and i == NT:
                    @pl.when(u == 0)
                    def _():
                        w_copy(1, 0, 0).wait()
                        for ahead in range(2):
                            w_copy(ahead, 1, 1).start()

                    for v in range(2, n):
                        @pl.when(u == v - 2)
                        def _():
                            y_copy(v).start()
                if opening and i == 2 * NT - 1:
                    @pl.when(u + 1 < n)
                    def _():
                        y_wait(u + 1)

                def after(p):
                    if p == 0:
                        if i < 2 * NT - 1:
                            push(u, (i + 1) % NT, (i + 1) % 2)
                        else:
                            push(nxt, 0, 0)
                    step = tile * PIECES + p - PIECES
                    if step >= 0 and step % SPREAD == SPREAD - 1 and step // SPREAD < PIECES:
                        drain(1 - kv, step // SPREAD, 1 - oslot if kv == 0 else oslot)

                feed(kv, slot, tile, i % 2, after)
            return place(layer, u), last

        carry = lax.fori_loop(0, n, lambda u, c: trip(0, u, c, True), (first, first))

        def layer_loop(layer, carry):
            slot = layer % 2
            for kv in range(2):
                w_copy(kv, layer, slot).wait()
            nl = jnp.minimum(layer + 1, L - 1)
            for kv in range(2):
                w_copy(kv, nl, 1 - slot).start()
            return lax.fori_loop(0, n, lambda u, c: trip(layer, u, c, False), carry)

        last, before = lax.fori_loop(1, L, layer_loop, carry)
        slot = (L * n - 1) % 2
        for kv in range(2):
            w_copy(kv, L - 1, L % 2).wait()
        out_copy(0, last, 0).wait()
        out_copy(1, last, 0).wait()
        out_copy(0, last, slot).start()
        out_copy(1, before, 1 - slot).start()
        for p in range(PIECES):
            drain(1, p, slot)
        for p in range(PIECES):
            for q in range(2):
                pltpu.matmul_acc_lhs(acc[0][q][p], jnp.zeros((ROWS, 256), jnp.bfloat16), load_staged_rhs=0 if p == 0 else None)
        out_copy(1, last, 0).wait()
        out_copy(1, last, slot).start()
        out_copy(0, last, 0).wait()
        out_copy(1, last, 0).wait()

    pl.run_scoped(run, *[pltpu.ACC(q)((ROWS, 256), jnp.float32) for _ in range(2) for q in range(2) for _ in range(PIECES)])


def project(sources, units, wk, wv, prev):
    n = len(units)
    out = jax.ShapeDtypeStruct((L, 6, HK, 4 * TOK), jnp.bfloat16)
    args = list(sources) + [wk, wv] + (list(prev) if prev else [])
    k = len(sources) + 2
    return pl.pallas_call(
        functools.partial(proj_body, units, len(sources), bool(prev)),
        out_shape=[out, out],
        in_specs=[pl.BlockSpec(memory_space=pl.ANY)] * len(args),
        out_specs=[pl.BlockSpec(memory_space=pl.ANY)] * 2,
        scratch_shapes=[
            pltpu.VMEM((n, TOK, D), jnp.bfloat16),
            pltpu.VMEM((2, 2, HK, D), jnp.bfloat16),
            pltpu.VMEM((2, 2, HK, TOK), jnp.bfloat16),
            pltpu.SemaphoreType.DMA((n,)),
            pltpu.SemaphoreType.DMA((2, 2)),
            pltpu.SemaphoreType.DMA((2,)),
        ],
        input_output_aliases={k: 0, k + 1: 1} if prev else {},
        cost_estimate=pl.CostEstimate(flops=2 * n * TOK * D * HK * 2 * L, bytes_accessed=n * (TOK * D * 2 + 2 * L * HK * TOK * 2) + 4 * L * HK * D, transcendentals=0),
        compiler_params=pltpu.CompilerParams(vmem_limit_bytes=67_000_000, has_side_effects=True),
    )(*args)


CHUNKS = ((0,), (1, 2, 3), (4,), (5,))
NORM_ROWS = 256


def blocks_of(name, *chunks):
    return [(name, c) for c in chunks]


PLAN = [
    (blocks_of("own", 0, 1, 2, 3), (0,)),
    (blocks_of("mate", 0, 1, 2, 3) + blocks_of("far", 0), (1,)),
    (blocks_of("far", 1) + blocks_of("fwd", 0), (2,)),
    (blocks_of("fwd", 1) + blocks_of("far", 2), (3,)),
    (blocks_of("far", 3) + blocks_of("fwd", 2), ()),
    (blocks_of("fwd", 3), ()),
]


def norm_body(x_ref, scale_ref, *outs):
    acts = x_ref[...].astype(jnp.float32)
    mean_sq = jnp.mean(acts * acts, axis=-1, keepdims=True)
    normed = (acts * lax.rsqrt(mean_sq + NORM_EPS) * scale_ref[...].astype(jnp.float32)).astype(jnp.bfloat16)
    block = pl.program_id(0)
    start = 0
    for seqs, out in zip(CHUNKS, outs):
        stop = start + len(seqs) * (TOK // NORM_ROWS)

        @pl.when((block >= start) & (block < stop))
        def _():
            out[...] = normed

        start = stop


def rms_norm(enc_out, norm_scale):
    per_seq = TOK // NORM_ROWS
    specs, start = [], 0
    for seqs in CHUNKS:
        blocks = len(seqs) * per_seq
        specs.append(pl.BlockSpec((1, NORM_ROWS, D), functools.partial(lambda start, blocks, i: (jnp.clip(i - start, 0, blocks - 1) // per_seq, jnp.clip(i - start, 0, blocks - 1) % per_seq, 0), start, blocks)))
        start += blocks
    return pl.pallas_call(
        norm_body,
        grid=(start,),
        out_shape=[jax.ShapeDtypeStruct((len(seqs), TOK, D), jnp.bfloat16) for seqs in CHUNKS],
        in_specs=[pl.BlockSpec((1, NORM_ROWS, D), lambda i: (i // per_seq, i % per_seq, 0)), pl.BlockSpec((1, 1, D), lambda i: (0, 0, 0))],
        out_specs=specs,
        cost_estimate=pl.CostEstimate(flops=start * NORM_ROWS * D * 6, bytes_accessed=start * NORM_ROWS * D * 4, transcendentals=0),
        compiler_params=pltpu.CompilerParams(vmem_limit_bytes=67_000_000),
    )(enc_out, norm_scale.reshape(1, 1, D))


def swap(x, code):
    return lax.ppermute(x, "tp", [(i, i ^ code) for i in range(4)])


def solution(mesh):
    def gather_and_project(enc_out, norm_scale, w_key, w_value):
        wk = jnp.transpose(w_key, (0, 2, 3, 1)).reshape(L, HK, D)
        wv = jnp.transpose(w_value, (0, 2, 3, 1)).reshape(L, HK, D)
        y = rms_norm(enc_out, norm_scale)
        count = len(CHUNKS)
        far = [swap(y[c], 2) for c in range(count)]
        mate = [swap(y[c], 1) for c in range(count)]
        fwd = [None] * count
        kept = {"own": y, "mate": mate, "far": far, "fwd": fwd}
        code = {"own": 0, "mate": 1, "far": 2, "fwd": 3}
        out = None
        for group, forward in PLAN:
            sources = [kept[name][c] for name, c in group]
            units = [(s, i, seq, code[name]) for s, (name, c) in enumerate(group) for i, seq in enumerate(CHUNKS[c])]
            out = project(sources, units, wk, wv, out)
            if forward:
                out, moved = lax.optimization_barrier((out, [far[c] for c in forward]))
                for c, block in zip(forward, moved):
                    far[c] = block
                    fwd[c] = swap(block, 1)
        return tuple(jnp.transpose(o.reshape(L, 6, 8, 64, 4 * TOK), (0, 1, 4, 2, 3)) for o in out)

    weight_spec = P(None, None, "tp", None)
    cache_spec = P(None, "dp", None, "tp", None)
    return jax.shard_map(gather_and_project, mesh=mesh, in_specs=(P("dp", "tp", None), P(None), weight_spec, weight_spec), out_specs=(cache_spec, cache_spec), check_vma=False)
```

```python
import functools
import jax, jax.numpy as jnp
from jax import lax
from jax.experimental import pallas as pl
from jax.experimental.pallas import tpu as pltpu

from jax.sharding import PartitionSpec as P

NORM_EPS = 1e-6
L, D, HK, TOK = 6, 2048, 512, 512
PIECES, ROWS = 8, 64
SPREAD = 2
NT = D // 256


def proj_body(units, n_src, has_prev, *refs):
    n = len(units)
    srcs = refs[:n_src]
    wk, wv = refs[n_src:n_src + 2]
    ok, ov = refs[n_src + 2 + (2 if has_prev else 0):n_src + 4 + (2 if has_prev else 0)]
    ybuf, wbuf, obuf, y_sem, w_sem, o_sem = refs[-6:]
    me = lax.axis_index("tp")

    def place(layer, u):
        seq, code = unit_scalars(u)
        return layer, seq, jnp.bitwise_xor(me, code) * TOK

    def out_copy(kv, at, slot):
        layer, seq, col = at
        dst = (ok, ov)[kv].at[layer, seq, :, pl.ds(pl.multiple_of(col, TOK), TOK)]
        return pltpu.make_async_copy(obuf.at[kv, slot], dst, o_sem.at[kv])

    def unit_scalars(u):
        seq, code = jnp.int32(units[0][2]), jnp.int32(units[0][3])
        for i in range(1, n):
            seq = jnp.where(u == i, units[i][2], seq)
            code = jnp.where(u == i, units[i][3], code)
        return seq, code

    def w_copy(kv, layer, slot):
        return pltpu.make_async_copy((wk, wv)[kv].at[layer], wbuf.at[slot, kv], w_sem.at[slot, kv])

    def y_copy(u):
        s, i = units[u][:2]
        return pltpu.make_async_copy(srcs[s].at[i], ybuf.at[u], y_sem.at[u])

    def y_wait(u):
        pltpu.make_async_copy(srcs[0].at[0], ybuf.at[u], y_sem.at[u]).wait()

    def run(*accs):
        acc = [[[accs[(kv * 2 + q) * PIECES + p] for p in range(PIECES)] for q in range(2)] for kv in range(2)]

        def push(u, tile, reg):
            for q in range(2):
                pltpu.matmul_push_rhs(ybuf[u, pl.ds(q * 256, 256), pl.ds(tile * 256, 256)], staging_register=reg, mxu_index=q, transpose=True)

        def feed(kv, slot, tile, reg, after):
            for p in range(PIECES):
                lhs = wbuf[slot, kv, pl.ds(p * ROWS, ROWS), pl.ds(tile * 256, 256)]
                for q in range(2):
                    pltpu.matmul_acc_lhs(acc[kv][q][p], lhs, load_staged_rhs=reg if p == 0 else None)
                after(p)

        def drain(kv, p, slot):
            for q in range(2):
                obuf[kv, slot, pl.ds(p * ROWS, ROWS), pl.ds(q * 256, 256)] = pltpu.matmul_pop(acc[kv][q][p]).astype(jnp.bfloat16)

        first = place(0, 0)
        w_copy(0, 0, 0).start()
        y_copy(0).start()
        w_copy(1, 0, 0).start()
        for kv in range(2):
            for p in range(PIECES):
                drain(kv, p, 1)
        out_copy(0, first, 0).start()
        out_copy(1, first, 0).start()
        w_copy(0, 0, 0).wait()
        y_copy(0).wait()
        push(0, 0, 1)
        for p in range(PIECES):
            for q in range(2):
                pltpu.matmul_acc_lhs(acc[1][q][p], jnp.zeros((ROWS, 256), jnp.bfloat16), load_staged_rhs=1 if p == 0 else None)
        push(0, 0, 0)
        for u in range(1, min(n, 2)):
            y_copy(u).start()

        def trip(layer, u, carry, opening):
            last, before = carry
            slot, oslot = layer % 2, (layer * n + u) % 2
            out_copy(0, last, 0).wait()
            out_copy(1, last, 0).wait()
            out_copy(0, last, 1 - oslot).start()
            out_copy(1, before, oslot).start()
            nxt = lax.select(u + 1 == n, 0, u + 1)
            for i in range(2 * NT):
                kv, tile = divmod(i, NT)
                if opening and i == NT:
                    @pl.when(u == 0)
                    def _():
                        w_copy(1, 0, 0).wait()
                        for ahead in range(2):
                            w_copy(ahead, 1, 1).start()

                    for v in range(2, n):
                        @pl.when(u == v - 2)
                        def _():
                            y_copy(v).start()
                if opening and i == 2 * NT - 1:
                    @pl.when(u + 1 < n)
                    def _():
                        y_wait(u + 1)

                def after(p):
                    if p == 0:
                        if i < 2 * NT - 1:
                            push(u, (i + 1) % NT, (i + 1) % 2)
                        else:
                            push(nxt, 0, 0)
                    step = tile * PIECES + p - PIECES
                    if step >= 0 and step % SPREAD == SPREAD - 1 and step // SPREAD < PIECES:
                        drain(1 - kv, step // SPREAD, 1 - oslot if kv == 0 else oslot)

                feed(kv, slot, tile, i % 2, after)
            return place(layer, u), last

        carry = lax.fori_loop(0, n, lambda u, c: trip(0, u, c, True), (first, first))

        def layer_loop(layer, carry):
            slot = layer % 2
            for kv in range(2):
                w_copy(kv, layer, slot).wait()
            nl = jnp.minimum(layer + 1, L - 1)
            for kv in range(2):
                w_copy(kv, nl, 1 - slot).start()
            return lax.fori_loop(0, n, lambda u, c: trip(layer, u, c, False), carry)

        last, before = lax.fori_loop(1, L, layer_loop, carry)
        slot = (L * n - 1) % 2
        for kv in range(2):
            w_copy(kv, L - 1, L % 2).wait()
        out_copy(0, last, 0).wait()
        out_copy(1, last, 0).wait()
        out_copy(0, last, slot).start()
        out_copy(1, before, 1 - slot).start()
        for p in range(PIECES):
            drain(1, p, slot)
        for p in range(PIECES):
            for q in range(2):
                pltpu.matmul_acc_lhs(acc[0][q][p], jnp.zeros((ROWS, 256), jnp.bfloat16), load_staged_rhs=0 if p == 0 else None)
        out_copy(1, last, 0).wait()
        out_copy(1, last, slot).start()
        out_copy(0, last, 0).wait()
        out_copy(1, last, 0).wait()

    pl.run_scoped(run, *[pltpu.ACC(q)((ROWS, 256), jnp.float32) for _ in range(2) for q in range(2) for _ in range(PIECES)])


def project(sources, units, wk, wv, prev):
    n = len(units)
    out = jax.ShapeDtypeStruct((L, 6, HK, 4 * TOK), jnp.bfloat16)
    args = list(sources) + [wk, wv] + (list(prev) if prev else [])
    k = len(sources) + 2
    return pl.pallas_call(
        functools.partial(proj_body, units, len(sources), bool(prev)),
        out_shape=[out, out],
        in_specs=[pl.BlockSpec(memory_space=pl.ANY)] * len(args),
        out_specs=[pl.BlockSpec(memory_space=pl.ANY)] * 2,
        scratch_shapes=[
            pltpu.VMEM((n, TOK, D), jnp.bfloat16),
            pltpu.VMEM((2, 2, HK, D), jnp.bfloat16),
            pltpu.VMEM((2, 2, HK, TOK), jnp.bfloat16),
            pltpu.SemaphoreType.DMA((n,)),
            pltpu.SemaphoreType.DMA((2, 2)),
            pltpu.SemaphoreType.DMA((2,)),
        ],
        input_output_aliases={k: 0, k + 1: 1} if prev else {},
        cost_estimate=pl.CostEstimate(flops=2 * n * TOK * D * HK * 2 * L, bytes_accessed=n * (TOK * D * 2 + 2 * L * HK * TOK * 2) + 4 * L * HK * D, transcendentals=0),
        compiler_params=pltpu.CompilerParams(vmem_limit_bytes=67_000_000, has_side_effects=True),
    )(*args)


CHUNKS = ((0,), (1, 2, 3), (4,), (5,))


def blocks_of(name, *chunks):
    return [(name, c) for c in chunks]


PLAN = [
    (blocks_of("own", 0, 1, 2, 3), (0,)),
    (blocks_of("mate", 0, 1, 2, 3) + blocks_of("far", 0), (1,)),
    (blocks_of("far", 1) + blocks_of("fwd", 0), (2,)),
    (blocks_of("fwd", 1), (3,)),
    (blocks_of("far", 2) + blocks_of("fwd", 2), ()),
    (blocks_of("far", 3) + blocks_of("fwd", 3), ()),
]


def rms_norm(enc_out, norm_scale):
    acts = enc_out.astype(jnp.float32)
    mean_sq = jnp.mean(acts * acts, axis=-1, keepdims=True)
    return (acts * lax.rsqrt(mean_sq + NORM_EPS) * norm_scale.astype(jnp.float32)).astype(jnp.bfloat16)


def swap(x, code):
    return lax.ppermute(x, "tp", [(i, i ^ code) for i in range(4)])


def solution(mesh):
    def gather_and_project(enc_out, norm_scale, w_key, w_value):
        wk = jnp.transpose(w_key, (0, 2, 3, 1)).reshape(L, HK, D)
        wv = jnp.transpose(w_value, (0, 2, 3, 1)).reshape(L, HK, D)
        y = [rms_norm(enc_out[seqs[0] : seqs[-1] + 1], norm_scale) for seqs in CHUNKS]
        count = len(CHUNKS)
        far = [swap(y[c], 2) for c in range(count)]
        mate = [swap(y[c], 1) for c in range(count)]
        fwd = [None] * count
        kept = {"own": y, "mate": mate, "far": far, "fwd": fwd}
        code = {"own": 0, "mate": 1, "far": 2, "fwd": 3}
        out = None
        for group, forward in PLAN:
            sources = [kept[name][c] for name, c in group]
            units = [(s, i, seq, code[name]) for s, (name, c) in enumerate(group) for i, seq in enumerate(CHUNKS[c])]
            out = project(sources, units, wk, wv, out)
            if forward:
                out, moved = lax.optimization_barrier((out, [far[c] for c in forward]))
                for c, block in zip(forward, moved):
                    far[c] = block
                    fwd[c] = swap(block, 1)
        return tuple(jnp.transpose(o.reshape(L, 6, 8, 64, 4 * TOK), (0, 1, 4, 2, 3)) for o in out)

    weight_spec = P(None, None, "tp", None)
    cache_spec = P(None, "dp", None, "tp", None)
    return jax.shard_map(gather_and_project, mesh=mesh, in_specs=(P("dp", "tp", None), P(None), weight_spec, weight_spec), out_specs=(cache_spec, cache_spec), check_vma=False)
```
